32 devices in a mesh: task: 2 (over x), batch: 16 (over z, y, core).
Axes of the slice: x: 2, y: 2, z: 4, core: 2. Of those that a mesh axis runs over, the one named last changes fastest.
Arguments:
- pooled: bfloat16 [12288, 3328], P('batch'), may hold values from -6 to 6
- gate_weight: bfloat16 [3328, 8, 4], P(None, 'task'), may hold values from -0.21875 to 0.21875
- w_first: bfloat16 [8, 3328, 1024], P('task', 'batch'), may hold values from -0.15625 to 0.15625
- w_second: bfloat16 [8, 1024, 512], P('task', 'batch'), may hold values from -0.25 to 0.25
- w_third: bfloat16 [8, 512, 256], P('task', 'batch'), may hold values from -0.375 to 0.375
- tower_hidden: bfloat16 [4, 256, 128], P('task'), may hold values from -0.5 to 0.5
- tower_out: bfloat16 [4, 128], P('task'), may hold values from -0.75 to 0.75
Outputs:
- task_logits: float32 [12288, 4], P('batch', 'task')
The draws below stay inside these ranges and needn't reach their ends.
All inputs are finite; a program needn't handle non-finite values.
Results may differ from the reference program's by a relative error of at most 0.02.
Values may be sent and summed in bfloat16 or wider, within the bound.
A program may use at most 128 MiB of HBM per device.

```python
import jax
import jax.numpy as jnp

H1 = 1024
H2 = 512
H3 = 256
TOWER = 128
TASKS = 4
D_IN = 3328
EXPERTS = 8
TOKENS = 12288


def steps_of(own_key, extent, shards, smallest, largest):
    def one(position, parts):
        heights = jax.random.uniform(jax.random.fold_in(jax.random.fold_in(own_key, 6), position), (parts,), jnp.float32, smallest / len(shards), largest / len(shards))
        return jnp.repeat(jnp.exp(heights), extent[position] // parts).reshape((-1,) + (1,) * (len(extent) - position - 1))

    loudness = one(*shards[0])
    for cut in shards[1:]:
        loudness = loudness * one(*cut)
    return loudness


def centred(key, extent, width, limit, shards=(), kind=jnp.bfloat16):
    gain = steps_of(key, extent, shards, -0.22, 0.18) if shards else 1.0
    values = jax.random.normal(key, extent, jnp.float32) * width * gain
    return jnp.minimum(jnp.maximum(values, -limit), limit).astype(kind)


def setup_inputs(seed: int = 0) -> dict:
    streams_of = jax.random.split(jax.random.key(seed), 8)
    return {
        "pooled": centred(streams_of[0], (TOKENS, D_IN), 1.0, 6.0, ((0, 16),)),
        "gate_weight": centred(streams_of[1], (D_IN, EXPERTS, TASKS), (D_IN // 4) ** -0.5, 0.21875, ((1, 2),)),
        "w_first": centred(streams_of[2], (EXPERTS, D_IN, H1), (D_IN // 2) ** -0.5, 0.15625, ((0, 2), (1, 16))),
        "w_second": centred(streams_of[3], (EXPERTS, H1, H2), (H1 // 2) ** -0.5, 0.25, ((0, 2), (1, 16))),
        "w_third": centred(streams_of[4], (EXPERTS, H2, H3), (H2 // 2) ** -0.5, 0.375, ((0, 2), (1, 16))),
        "tower_hidden": centred(streams_of[5], (TASKS, H3, TOWER), (H3 // 2) ** -0.5, 0.5, ((0, 2),)),
        "tower_out": centred(streams_of[6], (TASKS, TOWER), (TOWER // 2) ** -0.5, 0.75, ((0, 2),)),
    }


def reference(pooled, gate_weight, w_first, w_second, w_third, tower_hidden, tower_out):
    logits = jnp.dot(pooled, gate_weight.reshape(D_IN, EXPERTS * TASKS), preferred_element_type=jnp.float32)
    logits = logits.reshape(TOKENS, EXPERTS, TASKS)
    weights = jnp.exp(logits)
    total = jnp.sum(weights, axis=1)
    numer = jnp.zeros((TOKENS, TASKS, H3), jnp.float32)
    for expert_id in range(EXPERTS):
        first = jax.nn.relu(jnp.dot(pooled, w_first[expert_id], preferred_element_type=jnp.float32)).astype(jnp.bfloat16)
        second = jax.nn.relu(jnp.dot(first, w_second[expert_id], preferred_element_type=jnp.float32)).astype(jnp.bfloat16)
        expert_out = jax.nn.relu(jnp.dot(second, w_third[expert_id], preferred_element_type=jnp.float32)).astype(jnp.bfloat16)
        numer = numer + weights[:, expert_id, :][:, :, None] * expert_out.astype(jnp.float32)[:, None, :]
    mix = (numer / total[:, :, None]).astype(jnp.bfloat16)
    tower = jax.nn.relu(jnp.einsum("sth,thk->stk", mix.astype(jnp.float32), tower_hidden.astype(jnp.float32))).astype(jnp.bfloat16)
    return jnp.einsum("stk,tk->st", tower.astype(jnp.float32), tower_out.astype(jnp.float32))
```

```python
import jax
import jax.numpy as jnp
from jax import lax
from jax.sharding import PartitionSpec as P


def per_device(pooled, gate_weight, w_first, w_second, w_third, tower_hidden, tower_out):
    tok_rows = pooled.shape[0]
    width_in = pooled.shape[1]
    local_experts = w_first.shape[0]
    all_tasks = gate_weight.shape[2]
    own_tasks = tower_hidden.shape[0]
    gathered = lax.all_gather(w_first, "batch", axis=1, tiled=True)
    deep_rows, deep_width = w_second.shape[1], w_second.shape[2]
    last_rows, last_width = w_third.shape[1], w_third.shape[2]
    halves = deep_width // last_width
    packed = jnp.concatenate(
        [w_second[:, :, i * last_width : (i + 1) * last_width] for i in range(halves)] + [w_third],
        axis=1,
    )
    gathered, packed = lax.optimization_barrier((gathered, packed))
    packed = lax.all_gather(packed, "batch", axis=1, tiled=False)
    second_all = jnp.concatenate(
        [packed[:, :, i * deep_rows : (i + 1) * deep_rows] for i in range(halves)], axis=3
    ).reshape(local_experts, -1, deep_width)
    third_all = packed[:, :, halves * deep_rows :].reshape(local_experts, -1, last_width)
    summed = jnp.einsum("tr,erh->eth", pooled, gathered, preferred_element_type=jnp.float32)
    first = jax.nn.relu(summed).astype(jnp.bfloat16)
    logits = jnp.dot(
        pooled,
        gate_weight.reshape(width_in, local_experts * all_tasks),
        preferred_element_type=jnp.float32,
    )
    weights = jnp.exp(logits.reshape(tok_rows, local_experts, all_tasks))
    gate_total = jnp.sum(weights, axis=1)
    columns = first
    second = jax.nn.relu(
        jnp.einsum(
            "etr,erh->eth",
            columns,
            second_all,
            preferred_element_type=jnp.float32,
        )
    ).astype(jnp.bfloat16)
    columns = second
    expert_out = jax.nn.relu(
        jnp.einsum(
            "etr,erh->eth",
            columns,
            third_all,
            preferred_element_type=jnp.float32,
        )
    ).astype(jnp.bfloat16)
    numer = jnp.einsum("tek,eth->tkh", weights, expert_out.astype(jnp.float32))
    groups = all_tasks // own_tasks
    me = lax.axis_index("task")
    numer_own = lax.dynamic_slice_in_dim(numer, me * own_tasks, own_tasks, 1)
    total_own = lax.dynamic_slice_in_dim(gate_total, me * own_tasks, own_tasks, 1)
    for shift in range(1, groups):
        ring = [(i, (i + shift) % groups) for i in range(groups)]
        other = lax.rem(me + shift, groups) * own_tasks
        numer_sent = lax.dynamic_slice_in_dim(numer, other, own_tasks, 1).astype(jnp.bfloat16)
        total_sent = lax.dynamic_slice_in_dim(gate_total, other, own_tasks, 1)
        numer_own = numer_own + lax.ppermute(numer_sent, "task", ring).astype(jnp.float32)
        total_own = total_own + lax.ppermute(total_sent, "task", ring)
    mix = (numer_own / total_own[:, :, None]).astype(jnp.bfloat16)
    tower = jax.nn.relu(
        jnp.einsum("tkh,khm->tkm", mix, tower_hidden, preferred_element_type=jnp.float32)
    ).astype(jnp.bfloat16)
    return jnp.einsum("tkm,km->tk", tower, tower_out, preferred_element_type=jnp.float32)


def solution(mesh):
    placed = (
        P("batch", None),
        P(None, "task", None),
        P("task", "batch", None),
        P("task", "batch", None),
        P("task", "batch", None),
        P("task", None, None),
        P("task", None),
    )
    return jax.shard_map(
        per_device, mesh=mesh, in_specs=placed, out_specs=P("batch", "task"), check_vma=False
    )
```

```python
import functools

import jax
import jax.numpy as jnp
from jax import lax
from jax.experimental import pallas as pl
from jax.experimental.pallas import tpu as pltpu
from jax.sharding import PartitionSpec as P

MESH = pl.DeviceIdType.MESH
BF16, F32 = jnp.bfloat16, jnp.float32
VMEM_BYTES = 63 * 1024 * 1024


def dot(a, b):
    return jnp.dot(a, b, preferred_element_type=F32)


def fused_kernel(
    nb, tiles, deep_rows,
    pooled, gate, w_first, packed, tower_hidden, tower_out, out,
    buf, dbuf, first, outs, outs_rx, wts, wts_rx, acc,
    loc, recv, szp, szm, sy, ssib, brecv, bzp, bzm, by, bsib, xs, xr, ws, wr,
):
    t, b = lax.axis_index("task"), lax.axis_index("batch")
    nz = nb // 4
    z, y, c = b // 4, (b // 2) % 2, b % 2
    experts = outs.shape[0]
    tasks = tower_hidden.shape[0]
    chunks = buf.shape[0]
    wide = buf.shape[3]
    tile = pooled.shape[0] // tiles

    def at(zz, yy, cc):
        return zz * 4 + yy * 2 + cc

    across, sib = at(z, 1 - y, c), at(z, y, 1 - c)
    up, down = at(z + 1, y, c), at(z - 1, y, c)

    def own_copy(k):
        return pltpu.make_async_copy(
            w_first.at[k // 2, :, pl.ds(pl.multiple_of((k % 2) * wide, 128), wide)],
            buf.at[k, b], loc.at[k],
        )

    deep_copy = pltpu.make_async_copy(packed, dbuf.at[b], loc.at[chunks])
    deep_copy.start()

    @pl.loop(0, chunks)
    def _(k):
        own_copy(k).start()

    barrier = pltpu.get_barrier_semaphore()
    for peer in (across, sib, at((z + 1) % nz, y, c), at((z + nz - 1) % nz, y, c)):
        pl.semaphore_signal(barrier, inc=1, device_id=(t, peer), device_id_type=MESH)
    pl.semaphore_signal(barrier, inc=1, device_id=(1 - t, b), device_id_type=MESH)
    pl.semaphore_wait(barrier, 5)

    def move(k, slot, sem, dev):
        return pltpu.make_async_remote_copy(
            src_ref=buf.at[k, slot], dst_ref=buf.at[k, slot], send_sem=sem,
            recv_sem=recv.at[k, slot], device_id=(t, dev), device_id_type=MESH,
        )

    def bmove(slot, sem, dev):
        return pltpu.make_async_remote_copy(
            src_ref=dbuf.at[slot], dst_ref=dbuf.at[slot], send_sem=sem,
            recv_sem=brecv.at[slot], device_id=(t, dev), device_id_type=MESH,
        )

    def arrived(k, slot):
        move(k, slot, sy.at[0, 0], sib).wait_recv()

    def barrived(slot):
        bmove(slot, by.at[0], sib).wait_recv()

    def own_z(k):
        @pl.when(z < nz - 1)
        def _():
            move(k, b, szp.at[k, z], up).start()

        @pl.when(z > 0)
        def _():
            move(k, b, szm.at[k, z], down).start()

    def z_step(k, d):
        @pl.when(z >= d)
        def _():
            slot = at(z - d, y, c)
            arrived(k, slot)

            @pl.when(z < nz - 1)
            def _():
                move(k, slot, szp.at[k, z - d], up).start()

            move(k, slot, sy.at[k, z - d], across).start()
            move(k, slot, ssib.at[k, z - d], sib).start()

        @pl.when(z + d < nz)
        def _():
            slot = at(z + d, y, c)
            arrived(k, slot)

            @pl.when(z > 0)
            def _():
                move(k, slot, szm.at[k, z + d], down).start()

            move(k, slot, sy.at[k, z + d], across).start()
            move(k, slot, ssib.at[k, z + d], sib).start()

    def y_step(k):
        @pl.loop(0, nz)
        def _(zz):
            slot = at(zz, 1 - y, c)
            arrived(k, slot)
            move(k, slot, ssib.at[k, nz + zz], sib).start()

    def sib_wait(k):
        @pl.loop(0, nz * 2)
        def _(q):
            arrived(k, q * 2 + (1 - c))

    def b_send_z(slot, yy, zz):
        @pl.when(jnp.logical_and(z < nz - 1, zz <= z))
        def _():
            bmove(slot, bzp.at[yy, zz], up).start()

        @pl.when(jnp.logical_and(z > 0, zz >= z))
        def _():
            bmove(slot, bzm.at[yy, zz], down).start()

    deep_copy.wait()
    bmove(b, by.at[0], across).start()
    b_send_z(b, y, z)
    bmove(b, bsib.at[y, z], sib).start()

    @pl.loop(0, chunks)
    def _(k):
        own_copy(k).wait()
        move(k, b, sy.at[k, z], across).start()
        move(k, b, ssib.at[k, z], sib).start()

    barrived(across)
    b_send_z(across, 1 - y, z)
    bmove(across, bsib.at[1 - y, z], sib).start()
    own_z(0)

    for m in range(tiles):
        rows = pl.ds(m * tile, tile)
        wts[rows, :] = jnp.exp(dot(pooled[rows, :], gate[...]))
    w_move = pltpu.make_async_remote_copy(
        src_ref=wts, dst_ref=wts_rx, send_sem=ws.at[0], recv_sem=wr.at[0],
        device_id=(1 - t, b), device_id_type=MESH,
    )
    w_move.start()
    acc[...] = jnp.zeros_like(acc)

    for d in range(1, nz):
        for same in (True, False):
            yy = y if same else 1 - y

            @pl.when(z >= d)
            def _():
                slot = at(z - d, yy, c)
                barrived(slot)
                b_send_z(slot, yy, z - d)
                bmove(slot, bsib.at[yy, z - d], sib).start()

            @pl.when(z + d < nz)
            def _():
                slot = at(z + d, yy, c)
                barrived(slot)
                b_send_z(slot, yy, z + d)
                bmove(slot, bsib.at[yy, z + d], sib).start()

    @pl.loop(0, nz * 2)
    def _(q):
        barrived(q * 2 + (1 - c))

    w_move.wait_recv()

    def x_move(e, m):
        rows = pl.ds(m * tile, tile)
        return pltpu.make_async_remote_copy(
            src_ref=outs.at[e, rows], dst_ref=outs_rx.at[e, rows],
            send_sem=xs.at[e, m], recv_sem=xr.at[e, m],
            device_id=(1 - t, b), device_id_type=MESH,
        )

    def accumulate(w_ref, base, e, m, value):
        rows = pl.ds(m * tile, tile)
        w = w_ref[rows, :]
        lane = lax.broadcasted_iota(jnp.int32, w.shape, 1)
        value = value.astype(F32)
        for j in range(tasks):
            column = jnp.sum(
                jnp.where(lane == base + j * experts + e, w, 0.0), axis=1, keepdims=True
            )
            acc[j, rows, :] = acc[j, rows, :] + column * value

    def compute(k, m):
        rows = pl.ds(m * tile, tile)
        weights = buf[k].reshape(-1, wide)
        first[k % 2, rows, :] = jnp.maximum(dot(pooled[rows, :], weights), 0.0).astype(BF16)

        @pl.when(k % 2 == 1)
        def _():
            e = k // 2
            width = dbuf.shape[3]
            low, high = first[0, rows, :], first[1, rows, :]
            total = None
            pieces = (dbuf.shape[2] - 1) // deep_rows
            for h in range(pieces):
                w2 = dbuf[:, e, pl.ds(h * deep_rows, deep_rows), :].reshape(-1, width)
                second = dot(low, w2[:wide]) + dot(high, w2[wide:])
                second = jnp.maximum(second, 0.0).astype(BF16)
                w3 = dbuf[:, e, pl.ds(pieces * deep_rows, dbuf.shape[2] - pieces * deep_rows), :]
                w3 = w3.reshape(-1, width)[h * width : (h + 1) * width]
                part = dot(second, w3)
                total = part if total is None else total + part
            value = jnp.maximum(total, 0.0).astype(BF16)
            outs[e, rows, :] = value
            x_move(e, m).start()
            accumulate(wts, 0, e, m, value)

            @pl.when(e >= 1)
            def _():
                x_move(e - 1, m).wait_recv()
                accumulate(wts_rx, tasks * experts, e - 1, m, outs_rx[e - 1, rows, :])

    @pl.loop(0, chunks + 2)
    def _(i):
        @pl.when(i + 1 < chunks)
        def _():
            own_z(i + 1)

        @pl.when(i >= 2)
        def _():
            sib_wait(i - 2)

        for s in range(max(tiles, nz - 1)):
            if s < tiles:
                @pl.when(i >= 2)
                def _():
                    compute(i - 2, s)
            if s + 1 < nz:
                @pl.when(i < chunks)
                def _():
                    z_step(i, s + 1)

        @pl.when(jnp.logical_and(i >= 1, i <= chunks))
        def _():
            y_step(i - 1)

    for m in range(tiles):
        rows = pl.ds(m * tile, tile)
        x_move(experts - 1, m).wait_recv()
        accumulate(wts_rx, tasks * experts, experts - 1, m, outs_rx[experts - 1, rows, :])
        own, other = wts[rows, :], wts_rx[rows, :]
        lane = lax.broadcasted_iota(jnp.int32, own.shape, 1)
        for j in range(tasks):
            lo = j * experts
            hi = lo + tasks * experts
            mine = jnp.logical_and(lane >= lo, lane < lo + experts)
            theirs = jnp.logical_and(lane >= hi, lane < hi + experts)
            total = jnp.sum(
                jnp.where(mine, own, 0.0) + jnp.where(theirs, other, 0.0), axis=1, keepdims=True
            )
            mix = (acc[j, rows, :] / total).astype(BF16)
            tower = jnp.maximum(dot(mix, tower_hidden[j]), 0.0).astype(BF16).astype(F32)
            out[rows, j : j + 1] = jnp.sum(
                tower * tower_out[j : j + 1, :].astype(F32), axis=1, keepdims=True
            )

    w_move.wait_send()
    for m in range(tiles):
        @pl.loop(0, experts)
        def _(e):
            x_move(e, m).wait_send()

    bmove(b, by.at[0], across).wait_send()

    @pl.loop(0, nz)
    def _(zz):
        for yy in range(2):
            slot = at(zz, yy, c)
            bmove(slot, bsib.at[yy, zz], sib).wait_send()

            @pl.when(jnp.logical_and(z < nz - 1, zz <= z))
            def _():
                bmove(slot, bzp.at[yy, zz], up).wait_send()

            @pl.when(jnp.logical_and(z > 0, zz >= z))
            def _():
                bmove(slot, bzm.at[yy, zz], down).wait_send()

        slot = at(zz, y, c)

        @pl.loop(0, chunks)
        def _(k):
            move(k, slot, sy.at[k, zz], across).wait_send()
            move(k, slot, ssib.at[k, zz], sib).wait_send()
            move(k, slot, ssib.at[k, nz + zz], sib).wait_send()

            @pl.when(jnp.logical_and(z < nz - 1, zz <= z))
            def _():
                move(k, slot, szp.at[k, zz], up).wait_send()

            @pl.when(jnp.logical_and(z > 0, zz >= z))
            def _():
                move(k, slot, szm.at[k, zz], down).wait_send()


def fused(nb, pooled, gate_weight, w_first, w_second, w_third, tower_hidden, tower_out):
    tokens, width_in = pooled.shape
    experts, rows, h1 = w_first.shape
    tasks = tower_hidden.shape[0]
    all_tasks = gate_weight.shape[2]
    deep_rows, deep_width = w_second.shape[1:]
    last_rows, last_width = w_third.shape[1:]
    nz = nb // 4
    chunks, wide = experts * 2, h1 // 2
    tiles = 3 if tokens % (3 * 16) == 0 else 1
    me = lax.axis_index("task")
    gate = jnp.roll(gate_weight, -me * tasks, axis=2)
    gate = jnp.transpose(gate, (0, 2, 1)).reshape(width_in, all_tasks * experts)
    gate = jnp.pad(gate, ((0, 0), (0, 128 - all_tasks * experts)))
    packed = jnp.concatenate(
        [w_second[:, :, i : i + last_width] for i in range(0, deep_width, last_width)]
        + [w_third],
        axis=1,
    )
    dma = pltpu.SemaphoreType.DMA
    vmem = pl.BlockSpec(memory_space=pltpu.VMEM)
    anywhere = pl.BlockSpec(memory_space=pl.ANY)
    return pl.pallas_call(
        functools.partial(fused_kernel, nb, tiles, deep_rows),
        out_shape=jax.ShapeDtypeStruct((tokens, tasks), F32),
        in_specs=[vmem, vmem, anywhere, anywhere, vmem, vmem],
        out_specs=vmem,
        scratch_shapes=[
            pltpu.VMEM((chunks, nb, rows, wide), BF16),
            pltpu.VMEM((nb,) + packed.shape, BF16),
            pltpu.VMEM((2, tokens, wide), BF16),
            pltpu.VMEM((experts, tokens, last_width), BF16),
            pltpu.VMEM((experts, tokens, last_width), BF16),
            pltpu.VMEM((tokens, 128), F32),
            pltpu.VMEM((tokens, 128), F32),
            pltpu.VMEM((tasks, tokens, last_width), F32),
            dma((chunks + 1,)),
            dma((chunks, nb)),
            dma((chunks, nz)),
            dma((chunks, nz)),
            dma((chunks, nz)),
            dma((chunks, 2 * nz)),
            dma((nb,)),
            dma((2, nz)),
            dma((2, nz)),
            dma((1,)),
            dma((2, nz)),
            dma((experts, tiles)),
            dma((experts, tiles)),
            dma((1,)),
            dma((1,)),
        ],
        compiler_params=pltpu.CompilerParams(
            collective_id=0, has_side_effects=True, vmem_limit_bytes=VMEM_BYTES
        ),
    )(pooled, gate, w_first, packed, tower_hidden, tower_out)


def gathered_first(pooled, gate_weight, w_first, w_second, w_third, tower_hidden, tower_out):
    tok_rows = pooled.shape[0]
    width_in = pooled.shape[1]
    local_experts = w_first.shape[0]
    all_tasks = gate_weight.shape[2]
    own_tasks = tower_hidden.shape[0]
    gathered = lax.all_gather(w_first, "batch", axis=1, tiled=True)
    deep_rows, deep_width = w_second.shape[1], w_second.shape[2]
    last_rows, last_width = w_third.shape[1], w_third.shape[2]
    halves = deep_width // last_width
    packed = jnp.concatenate(
        [w_second[:, :, i * last_width : (i + 1) * last_width] for i in range(halves)] + [w_third],
        axis=1,
    )
    gathered, packed = lax.optimization_barrier((gathered, packed))
    packed = lax.all_gather(packed, "batch", axis=1, tiled=False)
    second_all = jnp.concatenate(
        [packed[:, :, i * deep_rows : (i + 1) * deep_rows] for i in range(halves)], axis=3
    ).reshape(local_experts, -1, deep_width)
    third_all = packed[:, :, halves * deep_rows :].reshape(local_experts, -1, last_width)
    summed = jnp.einsum("tr,erh->eth", pooled, gathered, preferred_element_type=jnp.float32)
    first = jax.nn.relu(summed).astype(jnp.bfloat16)
    logits = jnp.dot(
        pooled,
        gate_weight.reshape(width_in, local_experts * all_tasks),
        preferred_element_type=jnp.float32,
    )
    weights = jnp.exp(logits.reshape(tok_rows, local_experts, all_tasks))
    gate_total = jnp.sum(weights, axis=1)
    columns = first
    second = jax.nn.relu(
        jnp.einsum(
            "etr,erh->eth",
            columns,
            second_all,
            preferred_element_type=jnp.float32,
        )
    ).astype(jnp.bfloat16)
    columns = second
    expert_out = jax.nn.relu(
        jnp.einsum(
            "etr,erh->eth",
            columns,
            third_all,
            preferred_element_type=jnp.float32,
        )
    ).astype(jnp.bfloat16)
    numer = jnp.einsum("tek,eth->tkh", weights, expert_out.astype(jnp.float32))
    groups = all_tasks // own_tasks
    me = lax.axis_index("task")
    numer_own = lax.dynamic_slice_in_dim(numer, me * own_tasks, own_tasks, 1)
    total_own = lax.dynamic_slice_in_dim(gate_total, me * own_tasks, own_tasks, 1)
    for shift in range(1, groups):
        ring = [(i, (i + shift) % groups) for i in range(groups)]
        other = lax.rem(me + shift, groups) * own_tasks
        numer_sent = lax.dynamic_slice_in_dim(numer, other, own_tasks, 1).astype(jnp.bfloat16)
        total_sent = lax.dynamic_slice_in_dim(gate_total, other, own_tasks, 1)
        numer_own = numer_own + lax.ppermute(numer_sent, "task", ring).astype(jnp.float32)
        total_own = total_own + lax.ppermute(total_sent, "task", ring)
    mix = (numer_own / total_own[:, :, None]).astype(jnp.bfloat16)
    tower = jax.nn.relu(
        jnp.einsum("tkh,khm->tkm", mix, tower_hidden, preferred_element_type=jnp.float32)
    ).astype(jnp.bfloat16)
    return jnp.einsum("tkm,km->tk", tower, tower_out, preferred_element_type=jnp.float32)


def fits(mesh, pooled, gate_weight, w_first, w_second, w_third):
    even = all(w.shape[1] % 16 == 0 for w in (w_first, w_second, w_third))
    lanes = gate_weight.shape[1] * gate_weight.shape[2] <= 128
    return even and lanes and mesh.shape["task"] == 2 and mesh.shape["batch"] % 4 == 0


def solution(mesh):
    placed = (
        P("batch", None),
        P(None, "task", None),
        P("task", "batch", None),
        P("task", "batch", None),
        P("task", "batch", None),
        P("task", None, None),
        P("task", None),
    )

    def per_device(*args):
        if fits(mesh, *args[:5]):
            return fused(mesh.shape["batch"], *args)
        return gathered_first(*args)

    return jax.shard_map(
        per_device, mesh=mesh, in_specs=placed, out_specs=P("batch", "task"), check_vma=False
    )
```

```python
import functools

import jax
import jax.numpy as jnp
from jax import lax
from jax.experimental import pallas as pl
from jax.experimental.pallas import tpu as pltpu
from jax.sharding import PartitionSpec as P

MESH = pl.DeviceIdType.MESH
BF16, F32 = jnp.bfloat16, jnp.float32
VMEM_BYTES = 63 * 1024 * 1024


def dot(a, b):
    return jnp.dot(a, b, preferred_element_type=F32)


def fused_kernel(
    nb, tiles, deep_rows,
    pooled, gate, w_first, w_second, w_third, tower_hidden, tower_out, out,
    buf, dbuf, first, outs, outs_rx, wts, wts_rx, acc,
    loc, recv, szp, szm, sy, ssib, brecv, bzp, bzm, by, bsib, xs, xr, ws, wr,
):
    t, b = lax.axis_index("task"), lax.axis_index("batch")
    nz = nb // 4
    z, y, c = b // 4, (b // 2) % 2, b % 2
    experts = outs.shape[0]
    tasks = tower_hidden.shape[0]
    chunks = buf.shape[0]
    wide = buf.shape[3]
    tile = pooled.shape[0] // tiles

    def at(zz, yy, cc):
        return zz * 4 + yy * 2 + cc

    across, sib = at(z, 1 - y, c), at(z, y, 1 - c)
    up, down = at(z + 1, y, c), at(z - 1, y, c)

    def own_copy(k):
        return pltpu.make_async_copy(
            w_first.at[k // 2, :, pl.ds(pl.multiple_of((k % 2) * wide, 128), wide)],
            buf.at[k, b], loc.at[k],
        )

    pieces = w_second.shape[2] // w_third.shape[2]
    deep_copies = [
        pltpu.make_async_copy(
            w_second.at[:, :, pl.ds(h * w_third.shape[2], w_third.shape[2])],
            dbuf.at[b, :, pl.ds(h * deep_rows, deep_rows)], loc.at[chunks + h],
        )
        for h in range(pieces)
    ] + [
        pltpu.make_async_copy(
            w_third, dbuf.at[b, :, pl.ds(pieces * deep_rows, w_third.shape[1])],
            loc.at[chunks + pieces],
        )
    ]
    for copy in deep_copies:
        copy.start()

    @pl.loop(0, chunks)
    def _(k):
        own_copy(k).start()

    barrier = pltpu.get_barrier_semaphore()
    for peer in (across, sib, at((z + 1) % nz, y, c), at((z + nz - 1) % nz, y, c)):
        pl.semaphore_signal(barrier, inc=1, device_id=(t, peer), device_id_type=MESH)
    pl.semaphore_signal(barrier, inc=1, device_id=(1 - t, b), device_id_type=MESH)
    pl.semaphore_wait(barrier, 5)

    def move(k, slot, sem, dev):
        return pltpu.make_async_remote_copy(
            src_ref=buf.at[k, slot], dst_ref=buf.at[k, slot], send_sem=sem,
            recv_sem=recv.at[k, slot], device_id=(t, dev), device_id_type=MESH,
        )

    def bmove(slot, sem, dev):
        return pltpu.make_async_remote_copy(
            src_ref=dbuf.at[slot], dst_ref=dbuf.at[slot], send_sem=sem,
            recv_sem=brecv.at[slot], device_id=(t, dev), device_id_type=MESH,
        )

    def arrived(k, slot):
        move(k, slot, sy.at[0, 0], sib).wait_recv()

    def barrived(slot):
        bmove(slot, by.at[0], sib).wait_recv()

    def own_z(k):
        @pl.when(z < nz - 1)
        def _():
            move(k, b, szp.at[k, z], up).start()

        @pl.when(z > 0)
        def _():
            move(k, b, szm.at[k, z], down).start()

    def z_step(k, d):
        @pl.when(z >= d)
        def _():
            slot = at(z - d, y, c)
            arrived(k, slot)

            @pl.when(z < nz - 1)
            def _():
                move(k, slot, szp.at[k, z - d], up).start()

            move(k, slot, sy.at[k, z - d], across).start()
            move(k, slot, ssib.at[k, z - d], sib).start()

        @pl.when(z + d < nz)
        def _():
            slot = at(z + d, y, c)
            arrived(k, slot)

            @pl.when(z > 0)
            def _():
                move(k, slot, szm.at[k, z + d], down).start()

            move(k, slot, sy.at[k, z + d], across).start()
            move(k, slot, ssib.at[k, z + d], sib).start()

    def y_step(k):
        @pl.loop(0, nz)
        def _(zz):
            slot = at(zz, 1 - y, c)
            arrived(k, slot)
            move(k, slot, ssib.at[k, nz + zz], sib).start()

    def sib_wait(k):
        @pl.loop(0, nz * 2)
        def _(q):
            arrived(k, q * 2 + (1 - c))

    def b_send_z(slot, yy, zz):
        @pl.when(jnp.logical_and(z < nz - 1, zz <= z))
        def _():
            bmove(slot, bzp.at[yy, zz], up).start()

        @pl.when(jnp.logical_and(z > 0, zz >= z))
        def _():
            bmove(slot, bzm.at[yy, zz], down).start()

    for copy in deep_copies:
        copy.wait()
    bmove(b, by.at[0], across).start()
    b_send_z(b, y, z)
    bmove(b, bsib.at[y, z], sib).start()

    @pl.loop(0, chunks)
    def _(k):
        own_copy(k).wait()
        move(k, b, sy.at[k, z], across).start()
        move(k, b, ssib.at[k, z], sib).start()

    barrived(across)
    b_send_z(across, 1 - y, z)
    bmove(across, bsib.at[1 - y, z], sib).start()
    own_z(0)

    for m in range(tiles):
        rows = pl.ds(m * tile, tile)
        wts[rows, :] = jnp.exp(dot(pooled[rows, :], gate[...]))
    w_move = pltpu.make_async_remote_copy(
        src_ref=wts, dst_ref=wts_rx, send_sem=ws.at[0], recv_sem=wr.at[0],
        device_id=(1 - t, b), device_id_type=MESH,
    )
    w_move.start()
    acc[...] = jnp.zeros_like(acc)

    for d in range(1, nz):
        for same in (True, False):
            yy = y if same else 1 - y

            @pl.when(z >= d)
            def _():
                slot = at(z - d, yy, c)
                barrived(slot)
                b_send_z(slot, yy, z - d)
                bmove(slot, bsib.at[yy, z - d], sib).start()

            @pl.when(z + d < nz)
            def _():
                slot = at(z + d, yy, c)
                barrived(slot)
                b_send_z(slot, yy, z + d)
                bmove(slot, bsib.at[yy, z + d], sib).start()

    @pl.loop(0, nz * 2)
    def _(q):
        barrived(q * 2 + (1 - c))

    w_move.wait_recv()

    def x_move(e, m):
        rows = pl.ds(m * tile, tile)
        return pltpu.make_async_remote_copy(
            src_ref=outs.at[e, rows], dst_ref=outs_rx.at[e, rows],
            send_sem=xs.at[e, m], recv_sem=xr.at[e, m],
            device_id=(1 - t, b), device_id_type=MESH,
        )

    def accumulate(w_ref, base, e, m, value):
        rows = pl.ds(m * tile, tile)
        w = w_ref[rows, :]
        lane = lax.broadcasted_iota(jnp.int32, w.shape, 1)
        value = value.astype(F32)
        for j in range(tasks):
            column = jnp.sum(
                jnp.where(lane == base + j * experts + e, w, 0.0), axis=1, keepdims=True
            )
            acc[j, rows, :] = acc[j, rows, :] + column * value

    def compute(k, m):
        rows = pl.ds(m * tile, tile)
        weights = buf[k].reshape(-1, wide)
        first[k % 2, rows, :] = jnp.maximum(dot(pooled[rows, :], weights), 0.0).astype(BF16)

        @pl.when(k % 2 == 1)
        def _():
            e = k // 2
            width = dbuf.shape[3]
            low, high = first[0, rows, :], first[1, rows, :]
            total = None
            for h in range(pieces):
                w2 = dbuf[:, e, pl.ds(h * deep_rows, deep_rows), :].reshape(-1, width)
                second = dot(low, w2[:wide]) + dot(high, w2[wide:])
                second = jnp.maximum(second, 0.0).astype(BF16)
                w3 = dbuf[:, e, pl.ds(pieces * deep_rows, dbuf.shape[2] - pieces * deep_rows), :]
                w3 = w3.reshape(-1, width)[h * width : (h + 1) * width]
                part = dot(second, w3)
                total = part if total is None else total + part
            value = jnp.maximum(total, 0.0).astype(BF16)
            outs[e, rows, :] = value
            x_move(e, m).start()
            accumulate(wts, 0, e, m, value)

            @pl.when(e >= 1)
            def _():
                x_move(e - 1, m).wait_recv()
                accumulate(wts_rx, tasks * experts, e - 1, m, outs_rx[e - 1, rows, :])

    @pl.loop(0, chunks + 2)
    def _(i):
        @pl.when(i + 1 < chunks)
        def _():
            own_z(i + 1)

        @pl.when(i >= 2)
        def _():
            sib_wait(i - 2)

        for s in range(max(tiles, nz - 1)):
            if s < tiles:
                @pl.when(i >= 2)
                def _():
                    compute(i - 2, s)
            if s + 1 < nz:
                @pl.when(i < chunks)
                def _():
                    z_step(i, s + 1)

        @pl.when(jnp.logical_and(i >= 1, i <= chunks))
        def _():
            y_step(i - 1)

    for m in range(tiles):
        rows = pl.ds(m * tile, tile)
        x_move(experts - 1, m).wait_recv()
        accumulate(wts_rx, tasks * experts, experts - 1, m, outs_rx[experts - 1, rows, :])
        own, other = wts[rows, :], wts_rx[rows, :]
        lane = lax.broadcasted_iota(jnp.int32, own.shape, 1)
        for j in range(tasks):
            lo = j * experts
            hi = lo + tasks * experts
            mine = jnp.logical_and(lane >= lo, lane < lo + experts)
            theirs = jnp.logical_and(lane >= hi, lane < hi + experts)
            total = jnp.sum(
                jnp.where(mine, own, 0.0) + jnp.where(theirs, other, 0.0), axis=1, keepdims=True
            )
            mix = (acc[j, rows, :] / total).astype(BF16)
            tower = jnp.maximum(dot(mix, tower_hidden[j]), 0.0).astype(BF16).astype(F32)
            out[rows, j : j + 1] = jnp.sum(
                tower * tower_out[j : j + 1, :].astype(F32), axis=1, keepdims=True
            )

    w_move.wait_send()
    for m in range(tiles):
        @pl.loop(0, experts)
        def _(e):
            x_move(e, m).wait_send()

    bmove(b, by.at[0], across).wait_send()

    @pl.loop(0, nz)
    def _(zz):
        for yy in range(2):
            slot = at(zz, yy, c)
            bmove(slot, bsib.at[yy, zz], sib).wait_send()

            @pl.when(jnp.logical_and(z < nz - 1, zz <= z))
            def _():
                bmove(slot, bzp.at[yy, zz], up).wait_send()

            @pl.when(jnp.logical_and(z > 0, zz >= z))
            def _():
                bmove(slot, bzm.at[yy, zz], down).wait_send()

        slot = at(zz, y, c)

        @pl.loop(0, chunks)
        def _(k):
            move(k, slot, sy.at[k, zz], across).wait_send()
            move(k, slot, ssib.at[k, zz], sib).wait_send()
            move(k, slot, ssib.at[k, nz + zz], sib).wait_send()

            @pl.when(jnp.logical_and(z < nz - 1, zz <= z))
            def _():
                move(k, slot, szp.at[k, zz], up).wait_send()

            @pl.when(jnp.logical_and(z > 0, zz >= z))
            def _():
                move(k, slot, szm.at[k, zz], down).wait_send()


def fused(nb, pooled, gate_weight, w_first, w_second, w_third, tower_hidden, tower_out):
    tokens, width_in = pooled.shape
    experts, rows, h1 = w_first.shape
    tasks = tower_hidden.shape[0]
    all_tasks = gate_weight.shape[2]
    deep_rows, deep_width = w_second.shape[1:]
    last_rows, last_width = w_third.shape[1:]
    nz = nb // 4
    chunks, wide = experts * 2, h1 // 2
    tiles = 3 if tokens % (3 * 16) == 0 else 1
    me = lax.axis_index("task")
    gate = jnp.roll(gate_weight, -me * tasks, axis=2)
    gate = jnp.transpose(gate, (0, 2, 1)).reshape(width_in, all_tasks * experts)
    gate = jnp.pad(gate, ((0, 0), (0, 128 - all_tasks * experts)))
    pieces = deep_width // last_width
    packed_rows = pieces * deep_rows + last_rows
    dma = pltpu.SemaphoreType.DMA
    vmem = pl.BlockSpec(memory_space=pltpu.VMEM)
    anywhere = pl.BlockSpec(memory_space=pl.ANY)
    return pl.pallas_call(
        functools.partial(fused_kernel, nb, tiles, deep_rows),
        out_shape=jax.ShapeDtypeStruct((tokens, tasks), F32),
        in_specs=[vmem, vmem, anywhere, anywhere, anywhere, vmem, vmem],
        out_specs=vmem,
        scratch_shapes=[
            pltpu.VMEM((chunks, nb, rows, wide), BF16),
            pltpu.VMEM((nb, experts, packed_rows, last_width), BF16),
            pltpu.VMEM((2, tokens, wide), BF16),
            pltpu.VMEM((experts, tokens, last_width), BF16),
            pltpu.VMEM((experts, tokens, last_width), BF16),
            pltpu.VMEM((tokens, 128), F32),
            pltpu.VMEM((tokens, 128), F32),
            pltpu.VMEM((tasks, tokens, last_width), F32),
            dma((chunks + pieces + 1,)),
            dma((chunks, nb)),
            dma((chunks, nz)),
            dma((chunks, nz)),
            dma((chunks, nz)),
            dma((chunks, 2 * nz)),
            dma((nb,)),
            dma((2, nz)),
            dma((2, nz)),
            dma((1,)),
            dma((2, nz)),
            dma((experts, tiles)),
            dma((experts, tiles)),
            dma((1,)),
            dma((1,)),
        ],
        compiler_params=pltpu.CompilerParams(
            collective_id=0, has_side_effects=True, vmem_limit_bytes=VMEM_BYTES
        ),
    )(pooled, gate, w_first, w_second, w_third, tower_hidden, tower_out)


def gathered_first(pooled, gate_weight, w_first, w_second, w_third, tower_hidden, tower_out):
    tok_rows = pooled.shape[0]
    width_in = pooled.shape[1]
    local_experts = w_first.shape[0]
    all_tasks = gate_weight.shape[2]
    own_tasks = tower_hidden.shape[0]
    gathered = lax.all_gather(w_first, "batch", axis=1, tiled=True)
    deep_rows, deep_width = w_second.shape[1], w_second.shape[2]
    last_rows, last_width = w_third.shape[1], w_third.shape[2]
    halves = deep_width // last_width
    packed = jnp.concatenate(
        [w_second[:, :, i * last_width : (i + 1) * last_width] for i in range(halves)] + [w_third],
        axis=1,
    )
    gathered, packed = lax.optimization_barrier((gathered, packed))
    packed = lax.all_gather(packed, "batch", axis=1, tiled=False)
    second_all = jnp.concatenate(
        [packed[:, :, i * deep_rows : (i + 1) * deep_rows] for i in range(halves)], axis=3
    ).reshape(local_experts, -1, deep_width)
    third_all = packed[:, :, halves * deep_rows :].reshape(local_experts, -1, last_width)
    summed = jnp.einsum("tr,erh->eth", pooled, gathered, preferred_element_type=jnp.float32)
    first = jax.nn.relu(summed).astype(jnp.bfloat16)
    logits = jnp.dot(
        pooled,
        gate_weight.reshape(width_in, local_experts * all_tasks),
        preferred_element_type=jnp.float32,
    )
    weights = jnp.exp(logits.reshape(tok_rows, local_experts, all_tasks))
    gate_total = jnp.sum(weights, axis=1)
    columns = first
    second = jax.nn.relu(
        jnp.einsum(
            "etr,erh->eth",
            columns,
            second_all,
            preferred_element_type=jnp.float32,
        )
    ).astype(jnp.bfloat16)
    columns = second
    expert_out = jax.nn.relu(
        jnp.einsum(
            "etr,erh->eth",
            columns,
            third_all,
            preferred_element_type=jnp.float32,
        )
    ).astype(jnp.bfloat16)
    numer = jnp.einsum("tek,eth->tkh", weights, expert_out.astype(jnp.float32))
    groups = all_tasks // own_tasks
    me = lax.axis_index("task")
    numer_own = lax.dynamic_slice_in_dim(numer, me * own_tasks, own_tasks, 1)
    total_own = lax.dynamic_slice_in_dim(gate_total, me * own_tasks, own_tasks, 1)
    for shift in range(1, groups):
        ring = [(i, (i + shift) % groups) for i in range(groups)]
        other = lax.rem(me + shift, groups) * own_tasks
        numer_sent = lax.dynamic_slice_in_dim(numer, other, own_tasks, 1).astype(jnp.bfloat16)
        total_sent = lax.dynamic_slice_in_dim(gate_total, other, own_tasks, 1)
        numer_own = numer_own + lax.ppermute(numer_sent, "task", ring).astype(jnp.float32)
        total_own = total_own + lax.ppermute(total_sent, "task", ring)
    mix = (numer_own / total_own[:, :, None]).astype(jnp.bfloat16)
    tower = jax.nn.relu(
        jnp.einsum("tkh,khm->tkm", mix, tower_hidden, preferred_element_type=jnp.float32)
    ).astype(jnp.bfloat16)
    return jnp.einsum("tkm,km->tk", tower, tower_out, preferred_element_type=jnp.float32)


def fits(mesh, pooled, gate_weight, w_first, w_second, w_third):
    even = all(w.shape[1] % 16 == 0 for w in (w_first, w_second, w_third))
    lanes = gate_weight.shape[1] * gate_weight.shape[2] <= 128
    return even and lanes and mesh.shape["task"] == 2 and mesh.shape["batch"] % 4 == 0


def solution(mesh):
    placed = (
        P("batch", None),
        P(None, "task", None),
        P("task", "batch", None),
        P("task", "batch", None),
        P("task", "batch", None),
        P("task", None, None),
        P("task", None),
    )

    def per_device(*args):
        if fits(mesh, *args[:5]):
            return fused(mesh.shape["batch"], *args)
        return gathered_first(*args)

    return jax.shard_map(
        per_device, mesh=mesh, in_specs=placed, out_specs=P("batch", "task"), check_vma=False
    )
```
